128 devices in a mesh: dom: 128 (over x, z, y, core).
Axes of the slice: x: 4, y: 4, z: 4, core: 2. Of those that a mesh axis runs over, the one named last changes fastest.
Arguments:
- states: float32 [19, 524288], P(None, 'dom'), may hold values from 0 to 1
- region: int32 [524288], P('dom'), may hold values from 0 to 2
- half_volt: float32 [3, 18], replicated, may hold values from 0.2 to 0.8
- slopes: float32 [3, 18], replicated, may hold values from 0.05 to 0.2
- rates: float32 [3, 18], replicated, may hold values from 0.02 to 0.9
- conductance: float32 [3, 18], replicated, may hold values from 0.05 to 0.5
- reversal: float32 [3, 18], replicated, may hold values from -1 to 1
- stiffness: float32 [4096, 128, 128], P('dom'), as said below
- preconditioner: float32 [4096, 128, 128], P('dom'), as said below
- slots: int32 [524288], P('dom'), may hold values from 0 to 262143
- slot_gain: float32 [16384], replicated, may hold values from 0.5 to 2
- owner: int32 [524288, 1], P('dom'), may hold values from 0 to 127, as said below
- cell: int32 [524288], P('dom'), may hold values from 0 to 8191
- source_gain: float32 [524288], P('dom'), may hold values from 0.5 to 2
- torso_conduct: float32 [8192, 128], P('dom'), may hold values from 0.04 to 40
Outputs:
- new_states: float32 [19, 524288], P(None, 'dom')
- heart_potential: float32 [524288], P('dom')
- torso_potential: float32 [8192, 128], P('dom')
The draws below stay inside these ranges and needn't reach their ends.
Inputs may be any that keep to these rules, and one draw needn't show every extreme that they name: `slots`: slots of 16384 or more mark nodes off the interface. A heart node on device i has an owner among the eight torso devices i - 3 to i + 3 and i + 128 // 2 (indices wrapping around the axis); among the heart nodes of one device at most 1024 have the same owner, and that many do in every draw. `stiffness`: each tile's block is symmetric positive definite. `preconditioner`: each tile's block is the inverse of the stiffness block.
All inputs are finite; a program needn't handle non-finite values.
Results may differ from the reference program's by a relative error of at most 0.0001.
Values sent between devices are 32-bit elements; how exact they have to be, the bound alone decides.
No kernel may reach another device: no remote copies, remote signals or barrier semaphores. Data moves between devices by JAX's collectives and lax.ppermute only.
A program may use at most 64 MiB of HBM per device.

```python
import math
import jax
import jax.numpy as jnp
from jax import lax

STATES = 19
GATES = 18
REGIONS = 3
TR = 64
ITERS_H = 3
ITERS_T = 2
HN_DEV = 4096
HT = 4096
HN = 524288
NR = 8192
TN_DEV = 8192
NIF = 16384
CAP = 1024
N_DOM = 128


def tile_pair(key):
    base = jax.random.fold_in(key, 11)
    first, second = jax.random.split(base)
    rough = jax.random.normal(first, (HT, 128, 128), jnp.float32) * 0.06
    symmetric = rough + jnp.swapaxes(rough, 1, 2)
    diagonal = jax.random.uniform(second, (HT, 128), jnp.float32, 2.5, 4.5)
    matrices = symmetric + diagonal[:, :, None] * jnp.eye(128, dtype=jnp.float32)[None, :, :]
    return (matrices, jnp.linalg.inv(matrices))


def draw_stiffness(key, part):
    return tile_pair(key)[0]


def draw_preconditioner(key, part):
    return tile_pair(key)[1]


def draw_owner(key, part):
    base = jax.random.fold_in(key, 31)
    first, second = jax.random.split(base)
    keys = jax.random.split(first, N_DOM)
    order = jax.vmap(lambda single: jax.random.permutation(single, HN_DEV))(keys).astype(jnp.int32)
    leading = jax.random.randint(second, (N_DOM, 1), 0, 8).astype(jnp.int32)
    others = (leading + 1 + (order - CAP) % 7) % 8
    position = jnp.where(order < CAP, leading, others)
    delta = jnp.where(position == 7, N_DOM // 2, position - 3).astype(jnp.int32)
    device = jnp.arange(N_DOM, dtype=jnp.int32)[:, None]
    return ((device + delta + N_DOM) % N_DOM).reshape(N_DOM * HN_DEV, 1).astype(jnp.int32)


def draw_torso_conduct(key, part):
    first, second = jax.random.split(jax.random.fold_in(key, 23))
    factor = jnp.exp(jax.random.uniform(first, (N_DOM, 1, 1), jnp.float32) * jnp.log(20.0))
    spread = jnp.exp(jax.random.uniform(second, (N_DOM, TR, 128), jnp.float32) * jnp.log(40.0))
    return (0.05 * factor * spread).reshape(N_DOM * TR, 128)


def touch_ends(values, stream_key, low, top_value):
    place = [jax.random.randint(jax.random.fold_in(stream_key, axis), (), 0, length) for axis, length in enumerate(values.shape)]
    longest = values.shape.index(max(values.shape))
    next_to = place[:longest] + [(place[longest] + 1) % values.shape[longest]] + place[longest + 1:]
    return values.at[tuple(place)].set(low).at[tuple(next_to)].set(top_value)


def steps_of(stream_key, dims, shards, low, largest):
    gain = 1.0
    for dim, parts in shards:
        steps = jax.random.uniform(jax.random.fold_in(jax.random.fold_in(stream_key, 6), dim), (parts,), jnp.float32, low / len(shards), largest / len(shards))
        gain = gain * jnp.repeat(jnp.exp(steps), dims[dim] // parts).reshape((-1,) + (1,) * (len(dims) - 1 - dim))
    return gain


def setup_inputs(seed: int = 0) -> dict:
    arg_keys = jax.random.split(jax.random.key(seed), 16)
    states = jnp.clip(1.0 * jax.random.uniform(arg_keys[0], (STATES, HN), jnp.float32) ** steps_of(arg_keys[0], (STATES, HN), ((1, 128),), -0.2, 0.2), 0.0, 1.0)
    region = touch_ends(jax.random.randint(arg_keys[1], (HN,), 0, REGIONS), jax.random.fold_in(arg_keys[1], 1), 0, REGIONS - 1).astype(jnp.int32)
    half_volt = jnp.clip(jax.random.uniform(arg_keys[2], (REGIONS, GATES), jnp.float32, 0.2, 0.8), 0.2, 0.8)
    slopes = jnp.clip(jax.random.uniform(arg_keys[3], (REGIONS, GATES), jnp.float32, 0.05, 0.2), 0.05, 0.2)
    rates = jnp.clip(jnp.exp(jax.random.uniform(arg_keys[4], (REGIONS, GATES), jnp.float32, math.log(0.02), math.log(0.9))), 0.02, 0.9)
    conductance = jnp.clip(jnp.exp(jax.random.uniform(arg_keys[5], (REGIONS, GATES), jnp.float32, math.log(0.05), math.log(0.5))), 0.05, 0.5)
    reversal = jnp.clip(jax.random.uniform(arg_keys[6], (REGIONS, GATES), jnp.float32, -1.0, 1.0), -1.0, 1.0)
    stiffness = draw_stiffness(jax.random.fold_in(arg_keys[15], 71), 0)
    preconditioner = draw_preconditioner(jax.random.fold_in(arg_keys[15], 71), 0)
    slots = touch_ends(jax.random.randint(arg_keys[9], (HN,), 0, 16 * NIF), jax.random.fold_in(arg_keys[9], 1), 0, (16 * NIF) - 1).astype(jnp.int32)
    slot_gain = jnp.clip(jnp.exp(jax.random.uniform(arg_keys[10], (NIF,), jnp.float32, math.log(0.5), math.log(2.0))), 0.5, 2.0)
    owner = draw_owner(jax.random.fold_in(arg_keys[15], 71), 0)
    cell = touch_ends(jax.random.randint(arg_keys[12], (HN,), 0, TN_DEV), jax.random.fold_in(arg_keys[12], 1), 0, TN_DEV - 1).astype(jnp.int32)
    source_gain = jnp.clip(jnp.exp(math.log(2.0) - 1.3862944 * jax.random.uniform(arg_keys[13], (HN,), jnp.float32) ** steps_of(arg_keys[13], (HN,), ((0, 128),), -0.2, 0.2)), 0.5, 2.0)
    torso_conduct = draw_torso_conduct(jax.random.fold_in(arg_keys[15], 71), 0)
    return dict(states=states, region=region, half_volt=half_volt, slopes=slopes, rates=rates, conductance=conductance, reversal=reversal, stiffness=stiffness, preconditioner=preconditioner, slots=slots, slot_gain=slot_gain, owner=owner, cell=cell, source_gain=source_gain, torso_conduct=torso_conduct)


time_step = 0.2
heart_low = 1.0
heart_high = 4.0
highest = lax.Precision.HIGHEST

def ionic_step(states, region, half_volt, slopes, rates, conductance, reversal):
    volt = states[0]
    labels = (region[None, :] == jnp.arange(half_volt.shape[0], dtype=jnp.int32)[:, None]).astype(jnp.float32)

    def lookup(table):
        return jnp.dot(table.T, labels, precision=highest)
    target = jax.nn.sigmoid((volt[None, :] - lookup(half_volt)) / lookup(slopes))
    gates = target + (states[1:] - target) * jnp.exp(-lookup(rates))
    current = jnp.sum(lookup(conductance) * gates * (volt[None, :] - lookup(reversal)), axis=0)
    return jnp.concatenate([(volt - time_step * current)[None, :], gates], axis=0)

def tile_apply(mats, field):
    return jnp.einsum('tij,tj->ti', mats, field.reshape(-1, 128), precision=highest).reshape(-1)

def couple(field, slot_index, slot_gain):
    count = slot_gain.shape[0]
    partial_sum = jax.ops.segment_sum(field, slot_index, num_segments=count + 1)[:count]
    extended = jnp.concatenate([slot_gain * partial_sum, jnp.zeros((1,), jnp.float32)])
    return extended[slot_index]

def torso_apply(field, diagonal):
    padded = jnp.pad(field, 1)
    beside = padded[2:, 1:-1] + padded[:-2, 1:-1] + padded[1:-1, 2:] + padded[1:-1, :-2]
    return diagonal * field - beside

def reference(states, region, half_volt, slopes, rates, conductance, reversal, stiffness, preconditioner, slots, slot_gain, owner, cell, source_gain, torso_conduct):
    new_states = ionic_step(states, region, half_volt, slopes, rates, conductance, reversal)
    count = slot_gain.shape[0]
    slot_index = jnp.where(slots < count, slots, count).astype(jnp.int32)
    center = (heart_high + heart_low) / 2.0
    half_width = (heart_high - heart_low) / 2.0
    sigma_ratio = center / half_width
    resid = tile_apply(stiffness, new_states[0])
    update = tile_apply(preconditioner, resid) / center
    potential = update
    ratio_now = 1.0 / sigma_ratio
    for iteration in range(ITERS_H):
        resid = resid - (tile_apply(stiffness, update) + couple(update, slot_index, slot_gain))
        ratio_next = 1.0 / (2.0 * sigma_ratio - ratio_now)
        update = ratio_next * ratio_now * update + 2.0 * ratio_next / half_width * tile_apply(preconditioner, resid)
        potential = potential + update
        ratio_now = ratio_next
    deposit = potential * source_gain
    target_cell = (owner[:, 0] * TN_DEV + cell).astype(jnp.int32)
    source = jax.ops.segment_sum(deposit, target_cell, num_segments=NR * 128).reshape(NR, 128)
    diagonal = 4.0 + torso_conduct
    smallest = jnp.min(torso_conduct)
    low_bound = smallest / (4.0 + smallest)
    high_bound = (8.0 + smallest) / (4.0 + smallest)
    t_center = (high_bound + low_bound) / 2.0
    t_half = (high_bound - low_bound) / 2.0
    t_sigma = t_center / t_half
    t_resid = source
    t_update = t_resid / diagonal / t_center
    field = t_update
    t_ratio = 1.0 / t_sigma
    for iteration in range(ITERS_T):
        t_resid = t_resid - torso_apply(t_update, diagonal)
        t_next = 1.0 / (2.0 * t_sigma - t_ratio)
        t_update = t_next * t_ratio * t_update + 2.0 * t_next / t_half * (t_resid / diagonal)
        field = field + t_update
        t_ratio = t_next
    grounded = field - jnp.sum(field) / (NR * 128)
    return (new_states, potential, grounded)
```

```python
import jax
import jax.numpy as jnp
from jax import lax
from jax.experimental import pallas as pl
from jax.experimental.pallas import tpu as pltpu
from jax.sharding import Mesh
from jax.sharding import PartitionSpec as P

ITERS_H = 3
AXES = ("a", "b", "c", "d")
TIME_STEP = 0.2
CENTER = 2.5
HALF = 1.5
SIGMA = CENTER / HALF
F32 = jnp.float32
BF16 = jnp.bfloat16
TILES = 32
LANES = 128
SLOT_ROWS = 128
PAYLOAD = 136
TORSO = 64


def chebyshev_factors(count):
    ratio = 1.0 / SIGMA
    factors = []
    for _ in range(count):
        following = 1.0 / (2.0 * SIGMA - ratio)
        factors.append((following * ratio, 2.0 * following / HALF))
        ratio = following
    return factors


FACTORS = chebyshev_factors(ITERS_H)


def high_low(x):
    high = x.astype(BF16).astype(F32)
    return high, x - high


def tile_products(mats, x_ref, out_ref):
    lane = lax.broadcasted_iota(jnp.int32, (LANES, LANES), 1)
    columns = jnp.zeros((LANES, LANES), F32)
    for t in range(TILES):
        summed = jnp.sum(mats[t] * x_ref[t : t + 1, :], axis=1, keepdims=True)
        columns = jnp.where(lane == t, summed, columns)
    out_ref[...] = jnp.transpose(columns)[:TILES, :]


def slot_sums(slots_ref, w_ref, row_ref, col_ref):
    down = lax.broadcasted_iota(jnp.int32, (LANES, LANES), 0)
    for t in range(TILES):
        here = slice(t * LANES, (t + 1) * LANES)
        slot = slots_ref[t : t + 1, :]
        high, low = high_low(w_ref[t : t + 1, :])
        match = down == (slot >> 7)
        row_ref[0:LANES, here] = jnp.where(match, high, 0.0).astype(BF16)
        row_ref[LANES:, here] = jnp.where(match, low, 0.0).astype(BF16)
        col_ref[:, here] = jnp.where(down == (slot & 127), 1.0, 0.0).astype(BF16)
    both = lax.dot_general(
        row_ref[...], col_ref[...], (((1,), (1,)), ((), ())), preferred_element_type=F32
    )
    return both[:LANES] + both[LANES:]


def slot_values(slots_ref, values, pick_ref, out_ref):
    down = lax.broadcasted_iota(jnp.int32, (LANES, LANES), 0)
    high, low = high_low(jnp.transpose(values))
    table = jnp.concatenate([high.astype(BF16), low.astype(BF16)], axis=1)
    for t in range(TILES):
        here = slice(t * LANES, (t + 1) * LANES)
        match = jnp.where(down == (slots_ref[t : t + 1, :] >> 7), 1.0, 0.0).astype(BF16)
        pick_ref[0:LANES, here] = match
        pick_ref[LANES:, here] = match
    for t in range(TILES):
        here = slice(t * LANES, (t + 1) * LANES)
        rows = jnp.dot(table, pick_ref[:, here], preferred_element_type=F32)
        chosen = jnp.where(down == (slots_ref[t : t + 1, :] & 127), rows, 0.0)
        out_ref[t : t + 1, :] = jnp.sum(chosen, axis=0, keepdims=True)


def ionic_kernel(
    states_hbm, region_hbm, half_hbm, slope_hbm, rate_hbm, cond_hbm, rev_hbm,
    slots_hbm, conduct_hbm, gain_hbm, stiff_hbm, precond_hbm,
    states_out, resid_out, update_out, payload_out, slots_out, gain_out, stiff_out, precond_out,
    states_ref, region_ref, half_ref, slope_ref, rate_ref, cond_ref, rev_ref,
    conduct_ref, table_ref, volt_ref, row_ref, col_ref, sems,
):
    pairs = (
        (half_hbm, half_ref), (slope_hbm, slope_ref), (rate_hbm, rate_ref), (cond_hbm, cond_ref),
        (rev_hbm, rev_ref), (region_hbm, region_ref), (states_hbm, states_ref),
        (slots_hbm, slots_out), (conduct_hbm, conduct_ref),
        (stiff_hbm, stiff_out), (precond_hbm, precond_out), (gain_hbm, gain_out),
    )
    copies = [pltpu.make_async_copy(x, y, sems.at[k]) for k, (x, y) in enumerate(pairs)]
    for copy in copies:
        copy.start()
    table_ref[...] = jnp.zeros_like(table_ref)
    for copy in copies[:7]:
        copy.wait()
    for k, ref in enumerate((half_ref, slope_ref, rate_ref, cond_ref, rev_ref)):
        table_ref[8 * k : 8 * k + 3, 0:18] = ref[...]
    tables = jnp.transpose(pltpu.roll(table_ref[...], 1, 1))[:24]
    row = lax.broadcasted_iota(jnp.int32, (24, 1), 0)

    def column(k, r):
        return tables[:, 8 * k + r : 8 * k + r + 1]

    half = [column(0, r) for r in range(3)]
    gain = [1.0 / jnp.where((row == 0) | (row > 18), 1.0, column(1, r)) for r in range(3)]
    decay = [jnp.exp(-column(2, r)) for r in range(3)]
    cond = [column(3, r) for r in range(3)]
    rev = [column(4, r) for r in range(3)]
    first = lax.broadcasted_iota(jnp.int32, (19, LANES), 0) == 0
    for t in range(TILES):
        here = slice(t * LANES, (t + 1) * LANES)
        old = states_ref[:, here]
        volt = old[0:1, :]
        region = region_ref[t : t + 1, :]

        def lookup(choices):
            a, b, c = (x[:19] for x in choices)
            return jnp.where(region == 0, a, jnp.where(region == 1, b, c))

        target = 1.0 / (1.0 + jnp.exp((lookup(half) - volt) * lookup(gain)))
        gates = target + (old - target) * lookup(decay)
        flow = lookup(cond) * gates * (volt - lookup(rev))
        current = jnp.sum(jnp.where(first, 0.0, flow), axis=0, keepdims=True)
        new_volt = volt - TIME_STEP * current
        states_out[:, here] = jnp.where(first, new_volt, gates)
        volt_ref[t : t + 1, :] = new_volt
    for copy in copies[7:9]:
        copy.wait()
    payload_out[SLOT_ROWS:, :] = jnp.min(conduct_ref[...].reshape(8, 8, LANES), axis=0)
    copies[9].wait()
    tile_products(stiff_out, volt_ref, resid_out)
    copies[10].wait()
    tile_products(precond_out, resid_out, update_out)
    copies[11].wait()
    update_out[...] = update_out[...] * (1.0 / CENTER)
    payload_out[0:SLOT_ROWS, :] = slot_sums(slots_out, update_out, row_ref, col_ref)


def heart_step(
    index, payload_ref, gain_ref, slots_ref, stiff_ref, precond_ref, resid_ref, update_ref,
    potential_ref, coupled_ref, work_ref, pick_ref, resid_out, update_out, potential_out,
):
    slot_values(slots_ref, gain_ref[...] * payload_ref[0:SLOT_ROWS, :], pick_ref, coupled_ref)
    tile_products(stiff_ref, update_ref, work_ref)
    resid = resid_ref[...] - (work_ref[...] + coupled_ref[...])
    resid_out[...] = resid
    tile_products(precond_ref, resid_out, work_ref)
    keep, add = FACTORS[index]
    update = keep * update_ref[...] + add * work_ref[...]
    update_out[...] = update
    potential_out[...] = potential_ref[...] + update


def torso_solve(source_ref, conduct_ref, smallest, at_top, at_bottom):
    rows = TORSO + 16
    low = smallest / (4.0 + smallest)
    high = (8.0 + smallest) / (4.0 + smallest)
    center = (high + low) / 2.0
    half = (high - low) / 2.0
    sigma = center / half
    down = lax.broadcasted_iota(jnp.int32, (rows, LANES), 0)
    across = lax.broadcasted_iota(jnp.int32, (rows, LANES), 1)
    inside = ((down >= 8) | jnp.logical_not(at_top)) & ((down < 8 + TORSO) | jnp.logical_not(at_bottom))
    inside = inside & (down >= 6) & (down < 10 + TORSO)
    diagonal = 4.0 + conduct_ref
    inverse = 1.0 / diagonal

    def apply(u):
        u = jnp.where(inside, u, 0.0)
        up = pltpu.roll(u, 1, 0)
        dn = pltpu.roll(u, rows - 1, 0)
        left = jnp.where(across == 0, 0.0, pltpu.roll(u, 1, 1))
        right = jnp.where(across == LANES - 1, 0.0, pltpu.roll(u, LANES - 1, 1))
        return diagonal * u - (up + dn + left + right)

    resid = source_ref
    update = resid * inverse / center
    field = update
    ratio = 1.0 / sigma
    for _ in range(2):
        resid = resid - apply(update)
        following = 1.0 / (2.0 * sigma - ratio)
        update = following * ratio * update + 2.0 * following / half * (resid * inverse)
        field = field + update
        ratio = following
    return field


def first_step_kernel(
    here_ref, payload_ref, gain_ref, slots_ref, stiff_ref, precond_ref, resid_ref, update_ref, conduct_ref,
    resid_out, update_out, potential_out, payload_out, weight_out, smallest_out,
    coupled_ref, work_ref, pick_ref, row_ref, col_ref,
):
    heart_step(
        0, payload_ref, gain_ref, slots_ref, stiff_ref, precond_ref, resid_ref, update_ref,
        update_ref, coupled_ref, work_ref, pick_ref, resid_out, update_out, potential_out,
    )
    payload_out[...] = slot_sums(slots_ref, update_out, row_ref, col_ref)
    smallest = jnp.min(jnp.min(payload_ref[SLOT_ROWS:, :], axis=0, keepdims=True), axis=1, keepdims=True)
    smallest_out[...] = jnp.broadcast_to(smallest, (8, LANES))
    ones = jnp.ones((TORSO + 16, LANES), F32)
    field = torso_solve(
        ones, conduct_ref[...], smallest, here_ref[0] == 0, here_ref[0] == here_ref[1] - 1
    )
    weight_out[...] = field[8 : 8 + TORSO]


def second_step_kernel(
    payload_ref, gain_ref, slots_ref, stiff_ref, precond_ref, resid_ref, update_ref, potential_ref,
    resid_out, update_out, potential_out, payload_out,
    coupled_ref, work_ref, pick_ref, row_ref, col_ref,
):
    heart_step(
        1, payload_ref, gain_ref, slots_ref, stiff_ref, precond_ref, resid_ref, update_ref,
        potential_ref, coupled_ref, work_ref, pick_ref, resid_out, update_out, potential_out,
    )
    payload_out[...] = slot_sums(slots_ref, update_out, row_ref, col_ref)


def last_step_kernel(
    here_ref, payload_ref, gain_ref, slots_ref, stiff_ref, precond_ref, resid_ref, update_ref,
    potential_ref, owner_ref, cell_ref, scale_ref,
    potential_out, own_out, across_out, far_out, partner_out, next_out,
    coupled_ref, work_ref, pick_ref, resid_out, update_out, row_ref, col_ref,
):
    heart_step(
        2, payload_ref, gain_ref, slots_ref, stiff_ref, precond_ref, resid_ref, update_ref,
        potential_ref, coupled_ref, work_ref, pick_ref, resid_out, update_out, potential_out,
    )
    devices = here_ref[1]
    me = here_ref[0]
    ahead = owner_ref[...] - me + devices
    ahead = jnp.where(lax.rem(me, 2) == 1, ahead, 2 * devices - ahead)
    ahead = lax.rem(ahead, devices)
    kind = jnp.where(ahead == devices // 2, 1, 0)
    for k, value in ((2, 3), (3, devices - 1), (4, devices - 3), (5, devices - 2), (6, 2), (7, 1)):
        kind = jnp.where(ahead == value, k, kind)
    cell = cell_ref[...]
    row = (kind & 3) * TORSO + (cell >> 7)
    col = (kind >> 2) * LANES + (cell & 127)
    deposit = potential_out[...] * scale_ref[...]
    down = lax.broadcasted_iota(jnp.int32, (256, LANES), 0)
    for t in range(TILES):
        here = slice(t * LANES, (t + 1) * LANES)
        high, low = high_low(deposit[t : t + 1, :])
        match = down == row[t : t + 1, :]
        row_ref[0:256, here] = jnp.where(match, high, 0.0).astype(BF16)
        row_ref[256:, here] = jnp.where(match, low, 0.0).astype(BF16)
        col_ref[:, here] = jnp.where(down == col[t : t + 1, :], 1.0, 0.0).astype(BF16)
    both = lax.dot_general(
        row_ref[...], col_ref[...], (((1,), (1,)), ((), ())), preferred_element_type=F32
    )
    both = both[:256] + both[256:]

    def deposited(k):
        return both[(k % 4) * TORSO : (k % 4 + 1) * TORSO, (k // 4) * LANES : (k // 4 + 1) * LANES]

    own_out[...] = deposited(0)
    across_out[...] = deposited(1)
    far_out[...] = deposited(2)
    for k in range(3):
        partner_out[k * TORSO : (k + 1) * TORSO, :] = deposited(3 + k)
    for k in range(2):
        next_out[k * TORSO : (k + 1) * TORSO, :] = deposited(6 + k)


def source_kernel(
    here_ref, weight_ref, own_ref, across_ref, far_ref, partner_ref, next_ref, handed_ref,
    source_out, block_out,
):
    source = own_ref[...] + across_ref[...] + far_ref[...] + partner_ref[0:TORSO]
    source = source + next_ref[0:TORSO] + handed_ref[...]
    source_out[...] = source
    share = jnp.sum(jnp.sum(source * weight_ref[...], axis=0, keepdims=True), axis=1, keepdims=True)
    block_out[:, 0:LANES] = jnp.broadcast_to(share, (block_out.shape[0], LANES))
    peer = lax.broadcasted_iota(jnp.int32, (block_out.shape[0], LANES), 0)
    me = here_ref[0]
    for k in range(2):
        behind = jnp.where(peer == me - 1, source[k : k + 1], 0.0)
        ahead = jnp.where(peer == me + 1, source[TORSO - 2 + k : TORSO - 1 + k], behind)
        block_out[:, (1 + k) * LANES : (2 + k) * LANES] = ahead


def field_kernel(here_ref, block_ref, source_ref, conduct_ref, smallest_ref, out_ref, wide_ref):
    me = here_ref[0]
    devices = block_ref.shape[0]
    total = jnp.sum(jnp.sum(block_ref[:, 0:1], axis=0, keepdims=True), axis=1, keepdims=True)
    peer = lax.broadcasted_iota(jnp.int32, (devices, LANES), 0)
    wide_ref[...] = jnp.zeros_like(wide_ref)
    wide_ref[8 : 8 + TORSO, :] = source_ref[...]
    for k in range(2):
        rows = block_ref[:, (1 + k) * LANES : (2 + k) * LANES]
        above = jnp.sum(jnp.where(peer == me - 1, rows, 0.0), axis=0, keepdims=True)
        below = jnp.sum(jnp.where(peer == me + 1, rows, 0.0), axis=0, keepdims=True)
        wide_ref[6 + k : 7 + k, :] = above
        wide_ref[8 + TORSO + k : 9 + TORSO + k, :] = below
    field = torso_solve(
        wide_ref[...], conduct_ref[...], smallest_ref[0:1, 0:1], me == 0, me == devices - 1
    )
    out_ref[...] = field[8 : 8 + TORSO] - total * (1.0 / (devices * TORSO * LANES))


def call(kernel, outs, scratch, smem, flops, args, space=pltpu.VMEM):
    spec = [pl.BlockSpec(memory_space=pltpu.SMEM)] * smem
    if space == pltpu.HBM:
        args = [pltpu.with_memory_space_constraint(x, space) for x in args]
    spec += [pl.BlockSpec(memory_space=space)] * (len(args) - smem)
    return pl.pallas_call(
        kernel,
        out_shape=[s if isinstance(s, jax.ShapeDtypeStruct) else jax.ShapeDtypeStruct(s, F32) for s in outs],
        in_specs=spec,
        out_specs=[pl.BlockSpec(memory_space=pltpu.VMEM)] * len(outs),
        scratch_shapes=scratch,
        compiler_params=pltpu.CompilerParams(vmem_limit_bytes=16 * 1024 * 1024),
        cost_estimate=pl.CostEstimate(flops=flops, bytes_accessed=1 << 20, transcendentals=0),
    )(*args)


def place(i):
    return [i // 32, (i // 8) % 4, (i // 2) % 4, i % 2]


def index(c):
    return ((c[0] * 4 + c[1]) * 4 + c[2]) * 2 + c[3]


def permuted(x, move):
    return lax.ppermute(x, AXES, [(i, index(move(place(i)))) for i in range(128)])


def other_core(c):
    return c[:3] + [1 - c[3]]


def shifted(axis, by):
    def move(c):
        c = list(c)
        c[axis] = (c[axis] + by) % 4
        return c

    return move


def combined(parts, rows):
    total = parts[0]
    for part in parts[1:]:
        total = total + part
    if rows == SLOT_ROWS:
        return total
    least = parts[0]
    for part in parts[1:]:
        least = jnp.minimum(least, part)
    line = lax.broadcasted_iota(jnp.int32, total.shape, 0)
    return jnp.where(line < SLOT_ROWS, total, least)


def over_all(x):
    rows = x.shape[0]
    x = combined([x, permuted(x, other_core)], rows)
    for axis in range(3):
        x = combined([x] + [permuted(x, shifted(axis, k)) for k in (2, 1, 3)], rows)
    return x


def from_behind(x, by, count):
    return lax.ppermute(x, AXES, [(i, (i + by) % count) for i in range(count)])


def body(
    states, region, half_volt, slopes, rates, conductance, reversal, stiffness, preconditioner,
    slots, slot_gain, owner, cell, source_gain, torso_conduct,
):
    devices = lax.axis_size(AXES)
    here = lax.axis_index(AXES)
    node = (TILES, LANES)
    tile = (TORSO, LANES)
    grid = (SLOT_ROWS, LANES)
    region, slots, owner, cell, source_gain = (
        x.reshape(node) for x in (region, slots, owner, cell, source_gain)
    )
    gain = slot_gain.reshape(grid)
    whom = jnp.stack([here, jnp.int32(devices)]).astype(jnp.int32)
    mats = stiffness.shape
    rowspace = pltpu.VMEM((256, 4096), BF16)
    colspace = pltpu.VMEM((128, 4096), BF16)
    nodespace = pltpu.VMEM(node, F32)
    pickspace = pltpu.VMEM((256, 4096), BF16)
    tablespace = pltpu.VMEM((3, 18), F32)
    indexspace = pltpu.VMEM(node, jnp.int32)

    new_states, resid, update, payload, slots, gain, stiffness, preconditioner = call(
        ionic_kernel,
        [states.shape, node, node, (PAYLOAD, LANES), jax.ShapeDtypeStruct(node, jnp.int32), grid, mats, mats],
        [pltpu.VMEM(states.shape, F32), indexspace] + [tablespace] * 5
        + [pltpu.VMEM(tile, F32), pltpu.VMEM((128, 128), F32), nodespace, rowspace,
           colspace, pltpu.SemaphoreType.DMA((12,))],
        0, 40000000,
        (states, region, half_volt, slopes, rates, conductance, reversal, slots, torso_conduct,
         gain, stiffness, preconditioner),
        pltpu.HBM,
    )
    above = from_behind(torso_conduct[TORSO - 8 :], 1, devices)
    below = from_behind(torso_conduct[:8], -1, devices)
    conduct = jnp.concatenate([above, torso_conduct, below], axis=0)
    payload = over_all(payload)
    resid, update, potential, payload, weight, smallest = call(
        first_step_kernel,
        [node, node, node, grid, tile, (8, LANES)],
        [nodespace, nodespace, pickspace, rowspace, colspace],
        1, 40000000,
        (whom, payload, gain, slots, stiffness, preconditioner, resid, update, conduct),
    )
    payload = over_all(payload)
    resid, update, potential, payload = call(
        second_step_kernel,
        [node, node, node, grid],
        [nodespace, nodespace, pickspace, rowspace, colspace],
        0, 40000000,
        (payload, gain, slots, stiffness, preconditioner, resid, update, potential),
    )
    payload = over_all(payload)
    potential, own, across, far, partner, nearby = call(
        last_step_kernel,
        [node, tile, tile, tile, (3 * TORSO, LANES), (2 * TORSO, LANES)],
        [nodespace, nodespace, pickspace, nodespace, nodespace,
         pltpu.VMEM((512, 4096), BF16), pltpu.VMEM((256, 4096), BF16)],
        1, 40000000,
        (whom, payload, gain, slots, stiffness, preconditioner, resid, update, potential,
         owner, cell, source_gain),
    )
    partner = permuted(partner, other_core)
    far = lax.ppermute(far, AXES, [(i, (i + 3 if i % 2 else i - 3) % devices) for i in range(devices)])
    across = from_behind(across, devices // 2, devices)
    nearby = lax.ppermute(
        nearby + partner[TORSO:], AXES, [(i, (i + 2 if i % 2 else i - 2) % devices) for i in range(devices)]
    )
    handed = permuted(nearby[TORSO:], other_core)
    source, blocks = call(
        source_kernel,
        [tile, (devices, 3 * LANES)],
        [], 1, 1000000,
        (whom, weight, own, across, far, partner, nearby, handed),
    )
    blocks = lax.all_to_all(blocks, AXES, 0, 0, tiled=True)
    (grounded,) = call(
        field_kernel, [tile], [pltpu.VMEM((TORSO + 16, LANES), F32)], 1, 4000000,
        (whom, blocks, source, conduct, smallest),
    )
    return new_states, potential.reshape(-1), grounded


def solution(mesh):
    torus = Mesh(mesh.devices.reshape(4, 4, 4, 2), AXES)
    dom = P(AXES)
    placed = (
        P(None, AXES), dom, P(), P(), P(), P(), P(), P(AXES, None, None), P(AXES, None, None),
        dom, P(), P(AXES, None), dom, dom, P(AXES, None),
    )
    return jax.shard_map(
        body, mesh=torus, in_specs=placed, out_specs=(P(None, AXES), dom, P(AXES, None)), check_vma=False
    )
```

```python
import jax
import jax.numpy as jnp
from jax import lax
from jax.experimental import pallas as pl
from jax.experimental.pallas import tpu as pltpu
from jax.sharding import Mesh
from jax.sharding import PartitionSpec as P

ITERS_H = 3
AXES = ("a", "b", "c", "d")
TIME_STEP = 0.2
CENTER = 2.5
HALF = 1.5
SIGMA = CENTER / HALF
F32 = jnp.float32
BF16 = jnp.bfloat16
TILES = 32
LANES = 128
SLOT_ROWS = 128
PAYLOAD = 136
TORSO = 64


def chebyshev_factors(count):
    ratio = 1.0 / SIGMA
    factors = []
    for _ in range(count):
        following = 1.0 / (2.0 * SIGMA - ratio)
        factors.append((following * ratio, 2.0 * following / HALF))
        ratio = following
    return factors


FACTORS = chebyshev_factors(ITERS_H)


def high_low(x):
    high = x.astype(BF16).astype(F32)
    return high, x - high


def tile_products(mats, x_ref, out_ref):
    lane = lax.broadcasted_iota(jnp.int32, (LANES, LANES), 1)
    columns = jnp.zeros((LANES, LANES), F32)
    for t in range(TILES):
        summed = jnp.sum(mats[t] * x_ref[t : t + 1, :], axis=1, keepdims=True)
        columns = jnp.where(lane == t, summed, columns)
    out_ref[...] = jnp.transpose(columns)[:TILES, :]


def slot_sums(slots_ref, w_ref, row_ref, col_ref):
    down = lax.broadcasted_iota(jnp.int32, (LANES, LANES), 0)
    for t in range(TILES):
        here = slice(t * LANES, (t + 1) * LANES)
        slot = slots_ref[t : t + 1, :]
        high, low = high_low(w_ref[t : t + 1, :])
        match = down == (slot >> 7)
        row_ref[0:LANES, here] = jnp.where(match, high, 0.0).astype(BF16)
        row_ref[LANES:, here] = jnp.where(match, low, 0.0).astype(BF16)
        col_ref[:, here] = jnp.where(down == (slot & 127), 1.0, 0.0).astype(BF16)
    both = lax.dot_general(
        row_ref[...], col_ref[...], (((1,), (1,)), ((), ())), preferred_element_type=F32
    )
    return both[:LANES] + both[LANES:]


def slot_values(slots_ref, values, pick_ref, out_ref):
    down = lax.broadcasted_iota(jnp.int32, (LANES, LANES), 0)
    high, low = high_low(jnp.transpose(values))
    table = jnp.concatenate([high.astype(BF16), low.astype(BF16)], axis=1)
    for t in range(TILES):
        here = slice(t * LANES, (t + 1) * LANES)
        match = jnp.where(down == (slots_ref[t : t + 1, :] >> 7), 1.0, 0.0).astype(BF16)
        pick_ref[0:LANES, here] = match
        pick_ref[LANES:, here] = match
    for t in range(TILES):
        here = slice(t * LANES, (t + 1) * LANES)
        rows = jnp.dot(table, pick_ref[:, here], preferred_element_type=F32)
        chosen = jnp.where(down == (slots_ref[t : t + 1, :] & 127), rows, 0.0)
        out_ref[t : t + 1, :] = jnp.sum(chosen, axis=0, keepdims=True)


def ionic_kernel(
    states_hbm, region_hbm, half_hbm, slope_hbm, rate_hbm, cond_hbm, rev_hbm,
    slots_hbm, conduct_hbm, gain_hbm, precond_hbm,
    states_out, resid_out, update_out, payload_out, slots_out, gain_out, precond_out,
    states_ref, region_ref, half_ref, slope_ref, rate_ref, cond_ref, rev_ref,
    conduct_ref, table_ref, volt_ref, row_ref, col_ref, sems,
):
    pairs = (
        (half_hbm, half_ref), (slope_hbm, slope_ref), (rate_hbm, rate_ref), (cond_hbm, cond_ref),
        (rev_hbm, rev_ref), (region_hbm, region_ref), (states_hbm, states_ref),
        (slots_hbm, slots_out), (conduct_hbm, conduct_ref),
        (gain_hbm, gain_out), (precond_hbm, precond_out),
    )
    copies = [pltpu.make_async_copy(x, y, sems.at[k]) for k, (x, y) in enumerate(pairs)]
    for copy in copies:
        copy.start()
    table_ref[...] = jnp.zeros_like(table_ref)
    for copy in copies[:7]:
        copy.wait()
    for k, ref in enumerate((half_ref, slope_ref, rate_ref, cond_ref, rev_ref)):
        table_ref[8 * k : 8 * k + 3, 0:18] = ref[...]
    tables = jnp.transpose(pltpu.roll(table_ref[...], 1, 1))[:24]
    row = lax.broadcasted_iota(jnp.int32, (24, 1), 0)

    def column(k, r):
        return tables[:, 8 * k + r : 8 * k + r + 1]

    half = [column(0, r) for r in range(3)]
    gain = [1.0 / jnp.where((row == 0) | (row > 18), 1.0, column(1, r)) for r in range(3)]
    decay = [jnp.exp(-column(2, r)) for r in range(3)]
    cond = [column(3, r) for r in range(3)]
    rev = [column(4, r) for r in range(3)]
    first = lax.broadcasted_iota(jnp.int32, (19, LANES), 0) == 0
    for t in range(TILES):
        here = slice(t * LANES, (t + 1) * LANES)
        old = states_ref[:, here]
        volt = old[0:1, :]
        region = region_ref[t : t + 1, :]

        def lookup(choices):
            a, b, c = (x[:19] for x in choices)
            return jnp.where(region == 0, a, jnp.where(region == 1, b, c))

        target = 1.0 / (1.0 + jnp.exp((lookup(half) - volt) * lookup(gain)))
        gates = target + (old - target) * lookup(decay)
        flow = lookup(cond) * gates * (volt - lookup(rev))
        current = jnp.sum(jnp.where(first, 0.0, flow), axis=0, keepdims=True)
        new_volt = volt - TIME_STEP * current
        states_out[:, here] = jnp.where(first, new_volt, gates)
        volt_ref[t : t + 1, :] = new_volt
    for copy in copies[7:9]:
        copy.wait()
    payload_out[SLOT_ROWS:, :] = jnp.min(conduct_ref[...].reshape(8, 8, LANES), axis=0)
    volt = volt_ref[...]
    resid_out[...] = volt
    update_out[...] = volt * (1.0 / CENTER)
    payload_out[0:SLOT_ROWS, :] = slot_sums(slots_out, update_out, row_ref, col_ref)
    for copy in copies[9:]:
        copy.wait()


def heart_step(
    index, payload_ref, gain_ref, slots_ref, precond_ref, resid_ref, update_ref,
    potential_ref, coupled_ref, work_ref, pick_ref, resid_out, update_out, potential_out,
):
    slot_values(slots_ref, gain_ref[...] * payload_ref[0:SLOT_ROWS, :], pick_ref, coupled_ref)
    tile_products(precond_ref, coupled_ref, work_ref)
    resid = resid_ref[...] - (update_ref[...] + work_ref[...])
    resid_out[...] = resid
    keep, add = FACTORS[index]
    update = keep * update_ref[...] + add * resid
    update_out[...] = update
    potential_out[...] = potential_ref[...] + update


def torso_solve(source_ref, conduct_ref, smallest, at_top, at_bottom):
    rows = TORSO + 16
    low = smallest / (4.0 + smallest)
    high = (8.0 + smallest) / (4.0 + smallest)
    center = (high + low) / 2.0
    half = (high - low) / 2.0
    sigma = center / half
    down = lax.broadcasted_iota(jnp.int32, (rows, LANES), 0)
    across = lax.broadcasted_iota(jnp.int32, (rows, LANES), 1)
    inside = ((down >= 8) | jnp.logical_not(at_top)) & ((down < 8 + TORSO) | jnp.logical_not(at_bottom))
    inside = inside & (down >= 6) & (down < 10 + TORSO)
    diagonal = 4.0 + conduct_ref
    inverse = 1.0 / diagonal

    def apply(u):
        u = jnp.where(inside, u, 0.0)
        up = pltpu.roll(u, 1, 0)
        dn = pltpu.roll(u, rows - 1, 0)
        left = jnp.where(across == 0, 0.0, pltpu.roll(u, 1, 1))
        right = jnp.where(across == LANES - 1, 0.0, pltpu.roll(u, LANES - 1, 1))
        return diagonal * u - (up + dn + left + right)

    resid = source_ref
    update = resid * inverse / center
    field = update
    ratio = 1.0 / sigma
    for _ in range(2):
        resid = resid - apply(update)
        following = 1.0 / (2.0 * sigma - ratio)
        update = following * ratio * update + 2.0 * following / half * (resid * inverse)
        field = field + update
        ratio = following
    return field


def first_step_kernel(
    here_ref, payload_ref, gain_ref, slots_ref, precond_ref, resid_ref, update_ref, conduct_ref,
    resid_out, update_out, potential_out, payload_out, weight_out, smallest_out,
    coupled_ref, work_ref, pick_ref, row_ref, col_ref,
):
    heart_step(
        0, payload_ref, gain_ref, slots_ref, precond_ref, resid_ref, update_ref,
        update_ref, coupled_ref, work_ref, pick_ref, resid_out, update_out, potential_out,
    )
    payload_out[...] = slot_sums(slots_ref, update_out, row_ref, col_ref)
    smallest = jnp.min(jnp.min(payload_ref[SLOT_ROWS:, :], axis=0, keepdims=True), axis=1, keepdims=True)
    smallest_out[...] = jnp.broadcast_to(smallest, (8, LANES))
    ones = jnp.ones((TORSO + 16, LANES), F32)
    field = torso_solve(
        ones, conduct_ref[...], smallest, here_ref[0] == 0, here_ref[0] == here_ref[1] - 1
    )
    weight_out[...] = field[8 : 8 + TORSO]


def second_step_kernel(
    payload_ref, gain_ref, slots_ref, precond_ref, resid_ref, update_ref, potential_ref,
    resid_out, update_out, potential_out, payload_out,
    coupled_ref, work_ref, pick_ref, row_ref, col_ref,
):
    heart_step(
        1, payload_ref, gain_ref, slots_ref, precond_ref, resid_ref, update_ref,
        potential_ref, coupled_ref, work_ref, pick_ref, resid_out, update_out, potential_out,
    )
    payload_out[...] = slot_sums(slots_ref, update_out, row_ref, col_ref)


def last_step_kernel(
    here_ref, payload_ref, gain_ref, slots_ref, precond_ref, resid_ref, update_ref,
    potential_ref, owner_ref, cell_ref, scale_ref,
    potential_out, own_out, across_out, far_out, partner_out, next_out,
    coupled_ref, work_ref, pick_ref, resid_out, update_out, row_ref, col_ref,
):
    heart_step(
        2, payload_ref, gain_ref, slots_ref, precond_ref, resid_ref, update_ref,
        potential_ref, coupled_ref, work_ref, pick_ref, resid_out, update_out, potential_out,
    )
    devices = here_ref[1]
    me = here_ref[0]
    ahead = owner_ref[...] - me + devices
    ahead = jnp.where(lax.rem(me, 2) == 1, ahead, 2 * devices - ahead)
    ahead = lax.rem(ahead, devices)
    kind = jnp.where(ahead == devices // 2, 1, 0)
    for k, value in ((2, 3), (3, devices - 1), (4, devices - 3), (5, devices - 2), (6, 2), (7, 1)):
        kind = jnp.where(ahead == value, k, kind)
    cell = cell_ref[...]
    row = (kind & 3) * TORSO + (cell >> 7)
    col = (kind >> 2) * LANES + (cell & 127)
    deposit = potential_out[...] * scale_ref[...]
    down = lax.broadcasted_iota(jnp.int32, (256, LANES), 0)
    for t in range(TILES):
        here = slice(t * LANES, (t + 1) * LANES)
        high, low = high_low(deposit[t : t + 1, :])
        match = down == row[t : t + 1, :]
        row_ref[0:256, here] = jnp.where(match, high, 0.0).astype(BF16)
        row_ref[256:, here] = jnp.where(match, low, 0.0).astype(BF16)
        col_ref[:, here] = jnp.where(down == col[t : t + 1, :], 1.0, 0.0).astype(BF16)
    both = lax.dot_general(
        row_ref[...], col_ref[...], (((1,), (1,)), ((), ())), preferred_element_type=F32
    )
    both = both[:256] + both[256:]

    def deposited(k):
        return both[(k % 4) * TORSO : (k % 4 + 1) * TORSO, (k // 4) * LANES : (k // 4 + 1) * LANES]

    own_out[...] = deposited(0)
    across_out[...] = deposited(1)
    far_out[...] = deposited(2)
    for k in range(3):
        partner_out[k * TORSO : (k + 1) * TORSO, :] = deposited(3 + k)
    for k in range(2):
        next_out[k * TORSO : (k + 1) * TORSO, :] = deposited(6 + k)


def source_kernel(
    here_ref, weight_ref, own_ref, across_ref, far_ref, partner_ref, next_ref, handed_ref,
    source_out, block_out,
):
    source = own_ref[...] + across_ref[...] + far_ref[...] + partner_ref[0:TORSO]
    source = source + next_ref[0:TORSO] + handed_ref[...]
    source_out[...] = source
    share = jnp.sum(jnp.sum(source * weight_ref[...], axis=0, keepdims=True), axis=1, keepdims=True)
    block_out[:, 0:LANES] = jnp.broadcast_to(share, (block_out.shape[0], LANES))
    peer = lax.broadcasted_iota(jnp.int32, (block_out.shape[0], LANES), 0)
    me = here_ref[0]
    for k in range(2):
        behind = jnp.where(peer == me - 1, source[k : k + 1], 0.0)
        ahead = jnp.where(peer == me + 1, source[TORSO - 2 + k : TORSO - 1 + k], behind)
        block_out[:, (1 + k) * LANES : (2 + k) * LANES] = ahead


def field_kernel(here_ref, block_ref, source_ref, conduct_ref, smallest_ref, out_ref, wide_ref):
    me = here_ref[0]
    devices = block_ref.shape[0]
    total = jnp.sum(jnp.sum(block_ref[:, 0:1], axis=0, keepdims=True), axis=1, keepdims=True)
    peer = lax.broadcasted_iota(jnp.int32, (devices, LANES), 0)
    wide_ref[...] = jnp.zeros_like(wide_ref)
    wide_ref[8 : 8 + TORSO, :] = source_ref[...]
    for k in range(2):
        rows = block_ref[:, (1 + k) * LANES : (2 + k) * LANES]
        above = jnp.sum(jnp.where(peer == me - 1, rows, 0.0), axis=0, keepdims=True)
        below = jnp.sum(jnp.where(peer == me + 1, rows, 0.0), axis=0, keepdims=True)
        wide_ref[6 + k : 7 + k, :] = above
        wide_ref[8 + TORSO + k : 9 + TORSO + k, :] = below
    field = torso_solve(
        wide_ref[...], conduct_ref[...], smallest_ref[0:1, 0:1], me == 0, me == devices - 1
    )
    out_ref[...] = field[8 : 8 + TORSO] - total * (1.0 / (devices * TORSO * LANES))


def call(kernel, outs, scratch, smem, flops, args, space=pltpu.VMEM):
    spec = [pl.BlockSpec(memory_space=pltpu.SMEM)] * smem
    if space == pltpu.HBM:
        args = [pltpu.with_memory_space_constraint(x, space) for x in args]
    spec += [pl.BlockSpec(memory_space=space)] * (len(args) - smem)
    return pl.pallas_call(
        kernel,
        out_shape=[s if isinstance(s, jax.ShapeDtypeStruct) else jax.ShapeDtypeStruct(s, F32) for s in outs],
        in_specs=spec,
        out_specs=[pl.BlockSpec(memory_space=pltpu.VMEM)] * len(outs),
        scratch_shapes=scratch,
        compiler_params=pltpu.CompilerParams(vmem_limit_bytes=24 * 1024 * 1024),
        cost_estimate=pl.CostEstimate(flops=flops, bytes_accessed=1 << 20, transcendentals=0),
    )(*args)


def place(i):
    return [i // 32, (i // 8) % 4, (i // 2) % 4, i % 2]


def index(c):
    return ((c[0] * 4 + c[1]) * 4 + c[2]) * 2 + c[3]


def permuted(x, move):
    return lax.ppermute(x, AXES, [(i, index(move(place(i)))) for i in range(128)])


def other_core(c):
    return c[:3] + [1 - c[3]]


def shifted(axis, by):
    def move(c):
        c = list(c)
        c[axis] = (c[axis] + by) % 4
        return c

    return move


def combined(parts, rows):
    total = parts[0]
    for part in parts[1:]:
        total = total + part
    if rows == SLOT_ROWS:
        return total
    least = parts[0]
    for part in parts[1:]:
        least = jnp.minimum(least, part)
    line = lax.broadcasted_iota(jnp.int32, total.shape, 0)
    return jnp.where(line < SLOT_ROWS, total, least)


def over_all(x):
    rows = x.shape[0]
    x = combined([x, permuted(x, other_core)], rows)
    for axis in range(3):
        x = combined([x] + [permuted(x, shifted(axis, k)) for k in (2, 1, 3)], rows)
    return x


def from_behind(x, by, count):
    return lax.ppermute(x, AXES, [(i, (i + by) % count) for i in range(count)])


def body(
    states, region, half_volt, slopes, rates, conductance, reversal, stiffness, preconditioner,
    slots, slot_gain, owner, cell, source_gain, torso_conduct,
):
    devices = lax.axis_size(AXES)
    here = lax.axis_index(AXES)
    node = (TILES, LANES)
    tile = (TORSO, LANES)
    grid = (SLOT_ROWS, LANES)
    region, slots, owner, cell, source_gain = (
        x.reshape(node) for x in (region, slots, owner, cell, source_gain)
    )
    gain = slot_gain.reshape(grid)
    whom = jnp.stack([here, jnp.int32(devices)]).astype(jnp.int32)
    rowspace = pltpu.VMEM((256, 4096), BF16)
    colspace = pltpu.VMEM((128, 4096), BF16)
    nodespace = pltpu.VMEM(node, F32)
    pickspace = pltpu.VMEM((256, 4096), BF16)
    tablespace = pltpu.VMEM((3, 18), F32)
    indexspace = pltpu.VMEM(node, jnp.int32)

    new_states, resid, update, payload, slots, gain, preconditioner = call(
        ionic_kernel,
        [states.shape, node, node, (PAYLOAD, LANES), jax.ShapeDtypeStruct(node, jnp.int32), grid, preconditioner.shape],
        [pltpu.VMEM(states.shape, F32), indexspace] + [tablespace] * 5
        + [pltpu.VMEM(tile, F32), pltpu.VMEM((128, 128), F32), nodespace, rowspace,
           colspace, pltpu.SemaphoreType.DMA((11,))],
        0, 40000000,
        (states, region, half_volt, slopes, rates, conductance, reversal, slots, torso_conduct,
         gain, preconditioner),
        pltpu.HBM,
    )
    above = from_behind(torso_conduct[TORSO - 8 :], 1, devices)
    below = from_behind(torso_conduct[:8], -1, devices)
    conduct = jnp.concatenate([above, torso_conduct, below], axis=0)
    payload = over_all(payload)
    resid, update, potential, payload, weight, smallest = call(
        first_step_kernel,
        [node, node, node, grid, tile, (8, LANES)],
        [nodespace, nodespace, pickspace, rowspace, colspace],
        1, 40000000,
        (whom, payload, gain, slots, preconditioner, resid, update, conduct),
    )
    payload = over_all(payload)
    resid, update, potential, payload = call(
        second_step_kernel,
        [node, node, node, grid],
        [nodespace, nodespace, pickspace, rowspace, colspace],
        0, 40000000,
        (payload, gain, slots, preconditioner, resid, update, potential),
    )
    payload = over_all(payload)
    potential, own, across, far, partner, nearby = call(
        last_step_kernel,
        [node, tile, tile, tile, (3 * TORSO, LANES), (2 * TORSO, LANES)],
        [nodespace, nodespace, pickspace, nodespace, nodespace,
         pltpu.VMEM((512, 4096), BF16), pltpu.VMEM((256, 4096), BF16)],
        1, 40000000,
        (whom, payload, gain, slots, preconditioner, resid, update, potential,
         owner, cell, source_gain),
    )
    partner = permuted(partner, other_core)
    far = lax.ppermute(far, AXES, [(i, (i + 3 if i % 2 else i - 3) % devices) for i in range(devices)])
    across = from_behind(across, devices // 2, devices)
    nearby = lax.ppermute(
        nearby + partner[TORSO:], AXES, [(i, (i + 2 if i % 2 else i - 2) % devices) for i in range(devices)]
    )
    handed = permuted(nearby[TORSO:], other_core)
    source, blocks = call(
        source_kernel,
        [tile, (devices, 3 * LANES)],
        [], 1, 1000000,
        (whom, weight, own, across, far, partner, nearby, handed),
    )
    blocks = lax.all_to_all(blocks, AXES, 0, 0, tiled=True)
    (grounded,) = call(
        field_kernel, [tile], [pltpu.VMEM((TORSO + 16, LANES), F32)], 1, 4000000,
        (whom, blocks, source, conduct, smallest),
    )
    return new_states, potential.reshape(-1), grounded


def solution(mesh):
    torus = Mesh(mesh.devices.reshape(4, 4, 4, 2), AXES)
    dom = P(AXES)
    placed = (
        P(None, AXES), dom, P(), P(), P(), P(), P(), P(AXES, None, None), P(AXES, None, None),
        dom, P(), P(AXES, None), dom, dom, P(AXES, None),
    )
    return jax.shard_map(
        body, mesh=torus, in_specs=placed, out_specs=(P(None, AXES), dom, P(AXES, None)), check_vma=False
    )
```

```python
import jax
import jax.numpy as jnp
from jax import lax
from jax.experimental import pallas as pl
from jax.experimental.pallas import tpu as pltpu
from jax.sharding import Mesh
from jax.sharding import PartitionSpec as P

ITERS_H = 3
AXES = ("a", "b", "c", "d")
TIME_STEP = 0.2
CENTER = 2.5
HALF = 1.5
SIGMA = CENTER / HALF
F32 = jnp.float32
BF16 = jnp.bfloat16
TILES = 32
LANES = 128
SLOT_ROWS = 128
PAYLOAD = 136
TORSO = 64


def chebyshev_factors(count):
    ratio = 1.0 / SIGMA
    factors = []
    for _ in range(count):
        following = 1.0 / (2.0 * SIGMA - ratio)
        factors.append((following * ratio, 2.0 * following / HALF))
        ratio = following
    return factors


FACTORS = chebyshev_factors(ITERS_H)


def high_low(x):
    high = x.astype(BF16).astype(F32)
    return high, x - high


def tile_products(mats, x_ref, out_ref):
    lane = lax.broadcasted_iota(jnp.int32, (LANES, LANES), 1)
    columns = jnp.zeros((LANES, LANES), F32)
    for t in range(TILES):
        summed = jnp.sum(mats[t] * x_ref[t : t + 1, :], axis=1, keepdims=True)
        columns = jnp.where(lane == t, summed, columns)
    out_ref[...] = jnp.transpose(columns)[:TILES, :]


def one_hot_rows(slots_ref, pick_ref):
    down = lax.broadcasted_iota(jnp.int32, (LANES, LANES), 0)
    for t in range(TILES):
        here = slice(t * LANES, (t + 1) * LANES)
        match = down == (slots_ref[t : t + 1, :] >> 7)
        pick_ref[:, here] = jnp.where(match, 1.0, 0.0).astype(BF16)


def scaled_rows(w, pick_ref, count, row_ref):
    high, low = high_low(w)
    high, low = high.astype(BF16), low.astype(BF16)
    for t in range(TILES):
        here = slice(t * LANES, (t + 1) * LANES)
        row_ref[0:count, here] = pick_ref[0:count, here] * high[t : t + 1, :]
        row_ref[count:, here] = pick_ref[0:count, here] * low[t : t + 1, :]


def products(row_ref, col_ref, count):
    both = lax.dot_general(
        row_ref[...], col_ref[...], (((1,), (1,)), ((), ())), preferred_element_type=F32
    )
    return both[:count] + both[count:]


def slot_sums(slots_ref, w_ref, pick_ref, col_ref, row_ref):
    down = lax.broadcasted_iota(jnp.int32, (LANES, LANES), 0)
    for t in range(TILES):
        here = slice(t * LANES, (t + 1) * LANES)
        match = down == (slots_ref[t : t + 1, :] & 127)
        col_ref[:, here] = jnp.where(match, 1.0, 0.0).astype(BF16)
    scaled_rows(w_ref[...], pick_ref, LANES, row_ref)
    return products(row_ref, col_ref, LANES)


def slot_values(slots_ref, values, pick_ref, out_ref):
    down = lax.broadcasted_iota(jnp.int32, (LANES, LANES), 0)
    high, low = high_low(jnp.transpose(values))
    high, low = high.astype(BF16), low.astype(BF16)
    for t in range(TILES):
        here = slice(t * LANES, (t + 1) * LANES)
        rows = jnp.dot(high, pick_ref[:, here], preferred_element_type=F32)
        rows = rows + jnp.dot(low, pick_ref[:, here], preferred_element_type=F32)
        chosen = jnp.where(down == (slots_ref[t : t + 1, :] & 127), rows, 0.0)
        out_ref[t : t + 1, :] = jnp.sum(chosen, axis=0, keepdims=True)


def ionic_kernel(
    states_hbm, region_hbm, half_hbm, slope_hbm, rate_hbm, cond_hbm, rev_hbm,
    slots_hbm, conduct_hbm, gain_hbm, precond_hbm,
    states_out, resid_out, update_out, payload_out, slots_out, gain_out, precond_out,
    pick_out, top_out, bottom_out,
    states_ref, region_ref, half_ref, slope_ref, rate_ref, cond_ref, rev_ref,
    conduct_ref, table_ref, volt_ref, row_ref, col_ref, sems,
):
    pairs = (
        (half_hbm, half_ref), (slope_hbm, slope_ref), (rate_hbm, rate_ref), (cond_hbm, cond_ref),
        (rev_hbm, rev_ref), (region_hbm, region_ref), (states_hbm, states_ref),
        (slots_hbm, slots_out), (conduct_hbm, conduct_ref),
        (gain_hbm, gain_out), (precond_hbm, precond_out),
    )
    copies = [pltpu.make_async_copy(x, y, sems.at[k]) for k, (x, y) in enumerate(pairs)]
    for copy in copies:
        copy.start()
    table_ref[...] = jnp.zeros_like(table_ref)
    for copy in copies[:7]:
        copy.wait()
    for k, ref in enumerate((half_ref, slope_ref, rate_ref, cond_ref, rev_ref)):
        table_ref[8 * k : 8 * k + 3, 0:18] = ref[...]
    tables = jnp.transpose(pltpu.roll(table_ref[...], 1, 1))[:24]
    row = lax.broadcasted_iota(jnp.int32, (24, 1), 0)

    def column(k, r):
        return tables[:, 8 * k + r : 8 * k + r + 1]

    half = [column(0, r) for r in range(3)]
    gain = [1.0 / jnp.where((row == 0) | (row > 18), 1.0, column(1, r)) for r in range(3)]
    decay = [jnp.exp(-column(2, r)) for r in range(3)]
    cond = [column(3, r) for r in range(3)]
    rev = [column(4, r) for r in range(3)]
    first = lax.broadcasted_iota(jnp.int32, (19, LANES), 0) == 0
    for t in range(TILES):
        here = slice(t * LANES, (t + 1) * LANES)
        old = states_ref[:, here]
        volt = old[0:1, :]
        region = region_ref[t : t + 1, :]

        def lookup(choices):
            a, b, c = (x[:19] for x in choices)
            return jnp.where(region == 0, a, jnp.where(region == 1, b, c))

        target = 1.0 / (1.0 + jnp.exp((lookup(half) - volt) * lookup(gain)))
        gates = target + (old - target) * lookup(decay)
        flow = lookup(cond) * gates * (volt - lookup(rev))
        current = jnp.sum(jnp.where(first, 0.0, flow), axis=0, keepdims=True)
        new_volt = volt - TIME_STEP * current
        states_out[:, here] = jnp.where(first, new_volt, gates)
        volt_ref[t : t + 1, :] = new_volt
    for copy in copies[7:9]:
        copy.wait()
    top_out[...] = conduct_ref[0:8, :]
    bottom_out[...] = conduct_ref[TORSO - 8 :, :]
    payload_out[SLOT_ROWS:, :] = jnp.min(conduct_ref[...].reshape(8, 8, LANES), axis=0)
    volt = volt_ref[...]
    resid_out[...] = volt
    update_out[...] = volt * (1.0 / CENTER)
    one_hot_rows(slots_out, pick_out)
    payload_out[0:SLOT_ROWS, :] = slot_sums(
        slots_out, update_out, pick_out, col_ref, row_ref
    )
    for copy in copies[9:]:
        copy.wait()


def heart_step(
    index, payload_ref, gain_ref, slots_ref, precond_ref, resid_ref, update_ref,
    potential_ref, coupled_ref, work_ref, pick_ref, resid_out, update_out, potential_out,
):
    slot_values(slots_ref, gain_ref[...] * payload_ref[0:SLOT_ROWS, :], pick_ref, coupled_ref)
    tile_products(precond_ref, coupled_ref, work_ref)
    resid = resid_ref[...] - (update_ref[...] + work_ref[...])
    resid_out[...] = resid
    keep, add = FACTORS[index]
    update = keep * update_ref[...] + add * resid
    update_out[...] = update
    potential_out[...] = potential_ref[...] + update


def torso_solve(source_ref, conduct_ref, smallest, at_top, at_bottom):
    rows = TORSO + 16
    low = smallest / (4.0 + smallest)
    high = (8.0 + smallest) / (4.0 + smallest)
    center = (high + low) / 2.0
    half = (high - low) / 2.0
    sigma = center / half
    down = lax.broadcasted_iota(jnp.int32, (rows, LANES), 0)
    across = lax.broadcasted_iota(jnp.int32, (rows, LANES), 1)
    inside = ((down >= 8) | jnp.logical_not(at_top)) & ((down < 8 + TORSO) | jnp.logical_not(at_bottom))
    inside = inside & (down >= 6) & (down < 10 + TORSO)
    diagonal = 4.0 + conduct_ref
    inverse = 1.0 / diagonal

    def apply(u):
        u = jnp.where(inside, u, 0.0)
        up = pltpu.roll(u, 1, 0)
        dn = pltpu.roll(u, rows - 1, 0)
        left = jnp.where(across == 0, 0.0, pltpu.roll(u, 1, 1))
        right = jnp.where(across == LANES - 1, 0.0, pltpu.roll(u, LANES - 1, 1))
        return diagonal * u - (up + dn + left + right)

    resid = source_ref
    update = resid * inverse / center
    field = update
    ratio = 1.0 / sigma
    for _ in range(2):
        resid = resid - apply(update)
        following = 1.0 / (2.0 * sigma - ratio)
        update = following * ratio * update + 2.0 * following / half * (resid * inverse)
        field = field + update
        ratio = following
    return field


def first_step_kernel(
    here_ref, payload_ref, gain_ref, slots_ref, precond_ref, pick_ref, resid_ref, update_ref, conduct_ref,
    resid_out, update_out, potential_out, payload_out, weight_out, smallest_out,
    coupled_ref, work_ref, row_ref, col_ref,
):
    heart_step(
        0, payload_ref, gain_ref, slots_ref, precond_ref, resid_ref, update_ref,
        update_ref, coupled_ref, work_ref, pick_ref, resid_out, update_out, potential_out,
    )
    payload_out[...] = slot_sums(slots_ref, update_out, pick_ref, col_ref, row_ref)
    smallest = jnp.min(jnp.min(payload_ref[SLOT_ROWS:, :], axis=0, keepdims=True), axis=1, keepdims=True)
    smallest_out[...] = jnp.broadcast_to(smallest, (8, LANES))
    ones = jnp.ones((TORSO + 16, LANES), F32)
    field = torso_solve(
        ones, conduct_ref[...], smallest, here_ref[0] == 0, here_ref[0] == here_ref[1] - 1
    )
    weight_out[...] = field[8 : 8 + TORSO]


def second_step_kernel(
    payload_ref, gain_ref, slots_ref, precond_ref, pick_ref, resid_ref, update_ref, potential_ref,
    resid_out, update_out, potential_out, payload_out,
    coupled_ref, work_ref, row_ref, col_ref,
):
    heart_step(
        1, payload_ref, gain_ref, slots_ref, precond_ref, resid_ref, update_ref,
        potential_ref, coupled_ref, work_ref, pick_ref, resid_out, update_out, potential_out,
    )
    payload_out[...] = slot_sums(slots_ref, update_out, pick_ref, col_ref, row_ref)


def target_kernel(here_ref, after_ref, owner_ref, cell_ref, row_out, col_out):
    devices = here_ref[1]
    me = here_ref[0]
    ahead = owner_ref[...] - me + devices
    ahead = jnp.where(lax.rem(me, 2) == 1, ahead, 2 * devices - ahead)
    ahead = lax.rem(ahead, devices)
    kind = jnp.where(ahead == devices // 2, 1, 0)
    for k, value in ((2, 3), (3, devices - 1), (4, devices - 3), (5, devices - 2), (6, 2), (7, 1)):
        kind = jnp.where(ahead == value, k, kind)
    cell = cell_ref[...]
    row = (kind & 3) * TORSO + (cell >> 7)
    col = (kind >> 2) * LANES + (cell & 127)
    down = lax.broadcasted_iota(jnp.int32, (256, LANES), 0)
    for t in range(TILES):
        here = slice(t * LANES, (t + 1) * LANES)
        row_out[:, here] = jnp.where(down == row[t : t + 1, :], 1.0, 0.0).astype(BF16)
        col_out[:, here] = jnp.where(down == col[t : t + 1, :], 1.0, 0.0).astype(BF16)


def last_step_kernel(
    payload_ref, gain_ref, slots_ref, precond_ref, pick_ref, resid_ref, update_ref,
    potential_ref, to_row_ref, to_col_ref, scale_ref,
    potential_out, own_out, across_out, far_out, partner_out, next_out,
    coupled_ref, work_ref, resid_out, update_out, row_ref,
):
    heart_step(
        2, payload_ref, gain_ref, slots_ref, precond_ref, resid_ref, update_ref,
        potential_ref, coupled_ref, work_ref, pick_ref, resid_out, update_out, potential_out,
    )
    scaled_rows(potential_out[...] * scale_ref[...], to_row_ref, 256, row_ref)
    both = products(row_ref, to_col_ref, 256)

    def deposited(k):
        return both[(k % 4) * TORSO : (k % 4 + 1) * TORSO, (k // 4) * LANES : (k // 4 + 1) * LANES]

    own_out[...] = deposited(0)
    across_out[...] = deposited(1)
    far_out[...] = deposited(2)
    for k in range(3):
        partner_out[k * TORSO : (k + 1) * TORSO, :] = deposited(3 + k)
    for k in range(2):
        next_out[k * TORSO : (k + 1) * TORSO, :] = deposited(6 + k)


def source_kernel(
    here_ref, weight_ref, own_ref, across_ref, far_ref, partner_ref, next_ref, handed_ref,
    source_out, block_out,
):
    source = own_ref[...] + across_ref[...] + far_ref[...] + partner_ref[0:TORSO]
    source = source + next_ref[TORSO:] + handed_ref[...]
    source_out[...] = source
    share = jnp.sum(jnp.sum(source * weight_ref[...], axis=0, keepdims=True), axis=1, keepdims=True)
    block_out[:, 0:LANES] = jnp.broadcast_to(share, (block_out.shape[0], LANES))
    peer = lax.broadcasted_iota(jnp.int32, (block_out.shape[0], LANES), 0)
    me = here_ref[0]
    for k in range(2):
        behind = jnp.where(peer == me - 1, source[k : k + 1], 0.0)
        ahead = jnp.where(peer == me + 1, source[TORSO - 2 + k : TORSO - 1 + k], behind)
        block_out[:, (1 + k) * LANES : (2 + k) * LANES] = ahead


def field_kernel(here_ref, block_ref, source_ref, conduct_ref, smallest_ref, out_ref, wide_ref):
    me = here_ref[0]
    devices = block_ref.shape[0]
    total = jnp.sum(jnp.sum(block_ref[:, 0:1], axis=0, keepdims=True), axis=1, keepdims=True)
    peer = lax.broadcasted_iota(jnp.int32, (devices, LANES), 0)
    wide_ref[...] = jnp.zeros_like(wide_ref)
    wide_ref[8 : 8 + TORSO, :] = source_ref[...]
    for k in range(2):
        rows = block_ref[:, (1 + k) * LANES : (2 + k) * LANES]
        above = jnp.sum(jnp.where(peer == me - 1, rows, 0.0), axis=0, keepdims=True)
        below = jnp.sum(jnp.where(peer == me + 1, rows, 0.0), axis=0, keepdims=True)
        wide_ref[6 + k : 7 + k, :] = above
        wide_ref[8 + TORSO + k : 9 + TORSO + k, :] = below
    field = torso_solve(
        wide_ref[...], conduct_ref[...], smallest_ref[0:1, 0:1], me == 0, me == devices - 1
    )
    out_ref[...] = field[8 : 8 + TORSO] - total * (1.0 / (devices * TORSO * LANES))


def call(kernel, outs, scratch, smem, flops, args, space=pltpu.VMEM):
    spec = [pl.BlockSpec(memory_space=pltpu.SMEM)] * smem
    if space == pltpu.HBM:
        args = [pltpu.with_memory_space_constraint(x, space) for x in args]
    spec += [pl.BlockSpec(memory_space=space)] * (len(args) - smem)
    return pl.pallas_call(
        kernel,
        out_shape=[s if isinstance(s, jax.ShapeDtypeStruct) else jax.ShapeDtypeStruct(s, F32) for s in outs],
        in_specs=spec,
        out_specs=[pl.BlockSpec(memory_space=pltpu.VMEM)] * len(outs),
        scratch_shapes=scratch,
        compiler_params=pltpu.CompilerParams(vmem_limit_bytes=24 * 1024 * 1024),
        cost_estimate=pl.CostEstimate(flops=flops, bytes_accessed=1 << 20, transcendentals=0),
    )(*args)


def place(i):
    return [i // 32, (i // 8) % 4, (i // 2) % 4, i % 2]


def index(c):
    return ((c[0] * 4 + c[1]) * 4 + c[2]) * 2 + c[3]


def permuted(x, move):
    return lax.ppermute(x, AXES, [(i, index(move(place(i)))) for i in range(128)])


def other_core(c):
    return c[:3] + [1 - c[3]]


def swapped(axis, pairing):
    partner = ((1, 0, 3, 2), (3, 2, 1, 0), (2, 3, 0, 1))[pairing]

    def move(c):
        c = list(c)
        c[axis] = partner[c[axis]]
        return c

    return move


def combined(parts, rows):
    total = parts[0]
    for part in parts[1:]:
        total = total + part
    if rows == total.shape[0]:
        return total
    least = parts[0]
    for part in parts[1:]:
        least = jnp.minimum(least, part)
    line = lax.broadcasted_iota(jnp.int32, total.shape, 0)
    return jnp.where(line < rows, total, least)


def over_all(x):
    x = combined([x, permuted(x, other_core)], SLOT_ROWS)
    for axis in range(3):
        x = combined([x] + [permuted(x, swapped(axis, k)) for k in (0, 1, 2)], SLOT_ROWS)
    return x


def from_behind(x, by, count):
    return lax.ppermute(x, AXES, [(i, (i + by) % count) for i in range(count)])


def body(
    states, region, half_volt, slopes, rates, conductance, reversal, stiffness, preconditioner,
    slots, slot_gain, owner, cell, source_gain, torso_conduct,
):
    devices = lax.axis_size(AXES)
    here = lax.axis_index(AXES)
    node = (TILES, LANES)
    tile = (TORSO, LANES)
    grid = (SLOT_ROWS, LANES)
    region, slots, owner, cell, source_gain = (
        x.reshape(node) for x in (region, slots, owner, cell, source_gain)
    )
    gain = slot_gain.reshape(grid)
    whom = jnp.stack([here, jnp.int32(devices)]).astype(jnp.int32)
    rowspace = pltpu.VMEM((256, 4096), BF16)
    colspace = pltpu.VMEM((128, 4096), BF16)
    nodespace = pltpu.VMEM(node, F32)
    tablespace = pltpu.VMEM((3, 18), F32)
    indexspace = pltpu.VMEM(node, jnp.int32)

    pick = jax.ShapeDtypeStruct((128, 4096), BF16)
    target = jax.ShapeDtypeStruct((256, 4096), BF16)
    new_states, resid, update, payload, slots, gain, preconditioner, picks, top, bottom = call(
        ionic_kernel,
        [states.shape, node, node, (PAYLOAD, LANES), jax.ShapeDtypeStruct(node, jnp.int32), grid,
         preconditioner.shape, pick, (8, LANES), (8, LANES)],
        [pltpu.VMEM(states.shape, F32), indexspace] + [tablespace] * 5
        + [pltpu.VMEM(tile, F32), pltpu.VMEM((128, 128), F32), nodespace, rowspace,
           colspace, pltpu.SemaphoreType.DMA((11,))],
        0, 40000000,
        (states, region, half_volt, slopes, rates, conductance, reversal, slots, torso_conduct,
         gain, preconditioner),
        pltpu.HBM,
    )
    above = from_behind(bottom, 1, devices)
    below = from_behind(top, -1, devices)
    conduct = jnp.concatenate([above, torso_conduct, below], axis=0)
    payload = over_all(payload)
    resid, update, potential, payload, weight, smallest = call(
        first_step_kernel,
        [node, node, node, grid, tile, (8, LANES)],
        [nodespace, nodespace, rowspace, colspace],
        1, 40000000,
        (whom, payload, gain, slots, preconditioner, picks, resid, update, conduct),
    )
    to_row, to_col = call(
        target_kernel, [target, target], [], 1, 10000000, (whom, smallest, owner, cell)
    )
    payload = over_all(payload)
    resid, update, potential, payload = call(
        second_step_kernel,
        [node, node, node, grid],
        [nodespace, nodespace, rowspace, colspace],
        0, 40000000,
        (payload, gain, slots, preconditioner, picks, resid, update, potential),
    )
    payload = over_all(payload)
    potential, own, across, far, partner, nearby = call(
        last_step_kernel,
        [node, tile, tile, tile, (3 * TORSO, LANES), (2 * TORSO, LANES)],
        [nodespace, nodespace, nodespace, nodespace, pltpu.VMEM((512, 4096), BF16)],
        0, 40000000,
        (payload, gain, slots, preconditioner, picks, resid, update, potential,
         to_row, to_col, source_gain),
    )
    far = lax.ppermute(far, AXES, [(i, (i + 3 if i % 2 else i - 3) % devices) for i in range(devices)])
    across = from_behind(across, devices // 2, devices)
    partner = permuted(partner, other_core)
    nearby = lax.ppermute(
        nearby + partner[TORSO:], AXES, [(i, (i + 1 if i % 2 else i - 1) % devices) for i in range(devices)]
    )
    handed = permuted(nearby[:TORSO], other_core)
    source, blocks = call(
        source_kernel,
        [tile, (devices, 3 * LANES)],
        [], 1, 1000000,
        (whom, weight, own, across, far, partner, nearby, handed),
    )
    blocks = lax.all_to_all(blocks, AXES, 0, 0, tiled=True)
    (grounded,) = call(
        field_kernel, [tile], [pltpu.VMEM((TORSO + 16, LANES), F32)], 1, 4000000,
        (whom, blocks, source, conduct, smallest),
    )
    return new_states, potential.reshape(-1), grounded


def solution(mesh):
    torus = Mesh(mesh.devices.reshape(4, 4, 4, 2), AXES)
    dom = P(AXES)
    placed = (
        P(None, AXES), dom, P(), P(), P(), P(), P(), P(AXES, None, None), P(AXES, None, None),
        dom, P(), P(AXES, None), dom, dom, P(AXES, None),
    )
    return jax.shard_map(
        body, mesh=torus, in_specs=placed, out_specs=(P(None, AXES), dom, P(AXES, None)), check_vma=False
    )
```

```python
import jax
import jax.numpy as jnp
from jax import lax
from jax.experimental import pallas as pl
from jax.experimental.pallas import tpu as pltpu
from jax.sharding import Mesh
from jax.sharding import PartitionSpec as P

ITERS_H = 3
AXES = ("a", "b", "c", "d")
TIME_STEP = 0.2
CENTER = 2.5
HALF = 1.5
SIGMA = CENTER / HALF
F32 = jnp.float32
BF16 = jnp.bfloat16
TILES = 32
LANES = 128
SLOT_ROWS = 128
PAYLOAD = 136
TORSO = 64


def chebyshev_factors(count):
    ratio = 1.0 / SIGMA
    factors = []
    for _ in range(count):
        following = 1.0 / (2.0 * SIGMA - ratio)
        factors.append((following * ratio, 2.0 * following / HALF))
        ratio = following
    return factors


FACTORS = chebyshev_factors(ITERS_H)


def high_low(x):
    high = x.astype(BF16).astype(F32)
    return high, x - high


def tile_products(mats, x_ref, out_ref):
    lane = lax.broadcasted_iota(jnp.int32, (LANES, LANES), 1)
    columns = jnp.zeros((LANES, LANES), F32)
    for t in range(TILES):
        summed = jnp.sum(mats[t] * x_ref[t : t + 1, :], axis=1, keepdims=True)
        columns = jnp.where(lane == t, summed, columns)
    out_ref[...] = jnp.transpose(columns)[:TILES, :]


def one_hot_rows(slots_ref, pick_ref):
    down = lax.broadcasted_iota(jnp.int32, (LANES, LANES), 0)
    for t in range(TILES):
        here = slice(t * LANES, (t + 1) * LANES)
        match = down == (slots_ref[t : t + 1, :] >> 7)
        pick_ref[:, here] = jnp.where(match, 1.0, 0.0).astype(BF16)


def scaled_rows(w, pick_ref, count, row_ref):
    high, low = high_low(w)
    high, low = high.astype(BF16), low.astype(BF16)
    for t in range(TILES):
        here = slice(t * LANES, (t + 1) * LANES)
        row_ref[0:count, here] = pick_ref[0:count, here] * high[t : t + 1, :]
        row_ref[count:, here] = pick_ref[0:count, here] * low[t : t + 1, :]


def products(row_ref, col_ref, count):
    both = lax.dot_general(
        row_ref[...], col_ref[...], (((1,), (1,)), ((), ())), preferred_element_type=F32
    )
    return both[:count] + both[count:]


def one_hot_columns(slots_ref, col_ref):
    down = lax.broadcasted_iota(jnp.int32, (LANES, LANES), 0)
    for t in range(TILES):
        here = slice(t * LANES, (t + 1) * LANES)
        match = down == (slots_ref[t : t + 1, :] & 127)
        col_ref[:, here] = jnp.where(match, 1.0, 0.0).astype(BF16)


def slot_sums(w_ref, pick_ref, col_ref, row_ref):
    scaled_rows(w_ref[...], pick_ref, LANES, row_ref)
    return products(row_ref, col_ref, LANES)


def slot_values(slots_ref, values, pick_ref, out_ref):
    down = lax.broadcasted_iota(jnp.int32, (LANES, LANES), 0)
    high, low = high_low(jnp.transpose(values))
    high, low = high.astype(BF16), low.astype(BF16)
    for t in range(TILES):
        here = slice(t * LANES, (t + 1) * LANES)
        rows = jnp.dot(high, pick_ref[:, here], preferred_element_type=F32)
        rows = rows + jnp.dot(low, pick_ref[:, here], preferred_element_type=F32)
        chosen = jnp.where(down == (slots_ref[t : t + 1, :] & 127), rows, 0.0)
        out_ref[t : t + 1, :] = jnp.sum(chosen, axis=0, keepdims=True)


def ionic_kernel(
    states_hbm, region_hbm, half_hbm, slope_hbm, rate_hbm, cond_hbm, rev_hbm,
    slots_hbm, conduct_hbm, gain_hbm, precond_hbm,
    states_out, resid_out, update_out, payload_out, slots_out, gain_out, precond_out,
    pick_out, top_out, bottom_out,
    states_ref, region_ref, half_ref, slope_ref, rate_ref, cond_ref, rev_ref,
    conduct_ref, table_ref, volt_ref, row_ref, col_ref, sems,
):
    pairs = (
        (slots_hbm, slots_out), (half_hbm, half_ref), (slope_hbm, slope_ref), (rate_hbm, rate_ref),
        (cond_hbm, cond_ref), (rev_hbm, rev_ref), (region_hbm, region_ref), (states_hbm, states_ref),
        (conduct_hbm, conduct_ref),
        (gain_hbm, gain_out), (precond_hbm, precond_out),
    )
    copies = [pltpu.make_async_copy(x, y, sems.at[k]) for k, (x, y) in enumerate(pairs)]
    for copy in copies:
        copy.start()
    table_ref[...] = jnp.zeros_like(table_ref)
    copies[0].wait()
    one_hot_rows(slots_out, pick_out)
    one_hot_columns(slots_out, col_ref)
    for copy in copies[1:8]:
        copy.wait()
    for k, ref in enumerate((half_ref, slope_ref, rate_ref, cond_ref, rev_ref)):
        table_ref[8 * k : 8 * k + 3, 0:18] = ref[...]
    tables = jnp.transpose(pltpu.roll(table_ref[...], 1, 1))[:24]
    row = lax.broadcasted_iota(jnp.int32, (24, 1), 0)

    def column(k, r):
        return tables[:, 8 * k + r : 8 * k + r + 1]

    half = [column(0, r) for r in range(3)]
    gain = [1.0 / jnp.where((row == 0) | (row > 18), 1.0, column(1, r)) for r in range(3)]
    decay = [jnp.exp(-column(2, r)) for r in range(3)]
    cond = [column(3, r) for r in range(3)]
    rev = [column(4, r) for r in range(3)]
    first = lax.broadcasted_iota(jnp.int32, (19, LANES), 0) == 0
    for t in range(TILES):
        here = slice(t * LANES, (t + 1) * LANES)
        old = states_ref[:, here]
        volt = old[0:1, :]
        region = region_ref[t : t + 1, :]

        def lookup(choices):
            a, b, c = (x[:19] for x in choices)
            return jnp.where(region == 0, a, jnp.where(region == 1, b, c))

        target = 1.0 / (1.0 + jnp.exp((lookup(half) - volt) * lookup(gain)))
        gates = target + (old - target) * lookup(decay)
        flow = lookup(cond) * gates * (volt - lookup(rev))
        current = jnp.sum(jnp.where(first, 0.0, flow), axis=0, keepdims=True)
        new_volt = volt - TIME_STEP * current
        states_out[:, here] = jnp.where(first, new_volt, gates)
        volt_ref[t : t + 1, :] = new_volt
    copies[8].wait()
    top_out[...] = conduct_ref[0:8, :]
    bottom_out[...] = conduct_ref[TORSO - 8 :, :]
    payload_out[SLOT_ROWS:, :] = jnp.min(conduct_ref[...].reshape(8, 8, LANES), axis=0)
    volt = volt_ref[...]
    resid_out[...] = volt
    update_out[...] = volt * (1.0 / CENTER)
    payload_out[0:SLOT_ROWS, :] = slot_sums(update_out, pick_out, col_ref, row_ref)
    for copy in copies[9:]:
        copy.wait()


def heart_step(
    index, payload_ref, gain_ref, slots_ref, precond_ref, resid_ref, update_ref,
    potential_ref, coupled_ref, work_ref, pick_ref, resid_out, update_out, potential_out,
):
    slot_values(slots_ref, gain_ref[...] * payload_ref[0:SLOT_ROWS, :], pick_ref, coupled_ref)
    tile_products(precond_ref, coupled_ref, work_ref)
    resid = resid_ref[...] - (update_ref[...] + work_ref[...])
    resid_out[...] = resid
    keep, add = FACTORS[index]
    update = keep * update_ref[...] + add * resid
    update_out[...] = update
    potential_out[...] = potential_ref[...] + update


def torso_solve(source_ref, conduct_ref, smallest, at_top, at_bottom):
    rows = TORSO + 16
    low = smallest / (4.0 + smallest)
    high = (8.0 + smallest) / (4.0 + smallest)
    center = (high + low) / 2.0
    half = (high - low) / 2.0
    sigma = center / half
    down = lax.broadcasted_iota(jnp.int32, (rows, LANES), 0)
    across = lax.broadcasted_iota(jnp.int32, (rows, LANES), 1)
    inside = ((down >= 8) | jnp.logical_not(at_top)) & ((down < 8 + TORSO) | jnp.logical_not(at_bottom))
    inside = inside & (down >= 6) & (down < 10 + TORSO)
    diagonal = 4.0 + conduct_ref
    inverse = 1.0 / diagonal

    def apply(u):
        u = jnp.where(inside, u, 0.0)
        up = pltpu.roll(u, 1, 0)
        dn = pltpu.roll(u, rows - 1, 0)
        left = jnp.where(across == 0, 0.0, pltpu.roll(u, 1, 1))
        right = jnp.where(across == LANES - 1, 0.0, pltpu.roll(u, LANES - 1, 1))
        return diagonal * u - (up + dn + left + right)

    resid = source_ref
    update = resid * inverse / center
    field = update
    ratio = 1.0 / sigma
    for _ in range(2):
        resid = resid - apply(update)
        following = 1.0 / (2.0 * sigma - ratio)
        update = following * ratio * update + 2.0 * following / half * (resid * inverse)
        field = field + update
        ratio = following
    return field


def first_step_kernel(
    payload_ref, gain_ref, slots_ref, precond_ref, pick_ref, resid_ref, update_ref,
    resid_out, update_out, potential_out, payload_out, smallest_out,
    coupled_ref, work_ref, row_ref, col_ref,
):
    heart_step(
        0, payload_ref, gain_ref, slots_ref, precond_ref, resid_ref, update_ref,
        update_ref, coupled_ref, work_ref, pick_ref, resid_out, update_out, potential_out,
    )
    one_hot_columns(slots_ref, col_ref)
    payload_out[...] = slot_sums(update_out, pick_ref, col_ref, row_ref)
    smallest = jnp.min(jnp.min(payload_ref[SLOT_ROWS:, :], axis=0, keepdims=True), axis=1, keepdims=True)
    smallest_out[...] = jnp.broadcast_to(smallest, (8, LANES))


def weight_kernel(here_ref, smallest_ref, conduct_ref, weight_out):
    ones = jnp.ones((TORSO + 16, LANES), F32)
    field = torso_solve(
        ones, conduct_ref[...], smallest_ref[0:1, 0:1], here_ref[0] == 0, here_ref[0] == here_ref[1] - 1
    )
    weight_out[...] = field[8 : 8 + TORSO]


def second_step_kernel(
    payload_ref, gain_ref, slots_ref, precond_ref, pick_ref, resid_ref, update_ref, potential_ref,
    resid_out, update_out, potential_out, payload_out,
    coupled_ref, work_ref, row_ref, col_ref,
):
    heart_step(
        1, payload_ref, gain_ref, slots_ref, precond_ref, resid_ref, update_ref,
        potential_ref, coupled_ref, work_ref, pick_ref, resid_out, update_out, potential_out,
    )
    one_hot_columns(slots_ref, col_ref)
    payload_out[...] = slot_sums(update_out, pick_ref, col_ref, row_ref)


def target_kernel(here_ref, after_ref, owner_ref, cell_ref, row_out, col_out):
    devices = here_ref[1]
    me = here_ref[0]
    ahead = owner_ref[...] - me + devices
    ahead = jnp.where(lax.rem(me, 2) == 1, ahead, 2 * devices - ahead)
    ahead = lax.rem(ahead, devices)
    kind = jnp.where(ahead == devices // 2, 1, 0)
    for k, value in ((2, 3), (3, devices - 1), (4, devices - 3), (5, devices - 2), (6, 2), (7, 1)):
        kind = jnp.where(ahead == value, k, kind)
    cell = cell_ref[...]
    row = (kind & 3) * TORSO + (cell >> 7)
    col = (kind >> 2) * LANES + (cell & 127)
    down = lax.broadcasted_iota(jnp.int32, (256, LANES), 0)
    for t in range(TILES):
        here = slice(t * LANES, (t + 1) * LANES)
        row_out[:, here] = jnp.where(down == row[t : t + 1, :], 1.0, 0.0).astype(BF16)
        col_out[:, here] = jnp.where(down == col[t : t + 1, :], 1.0, 0.0).astype(BF16)


def last_step_kernel(
    payload_ref, gain_ref, slots_ref, precond_ref, pick_ref, resid_ref, update_ref,
    potential_ref, to_row_ref, to_col_ref, scale_ref,
    potential_out, own_out, across_out, far_out, partner_out, next_out,
    coupled_ref, work_ref, resid_out, update_out, row_ref,
):
    heart_step(
        2, payload_ref, gain_ref, slots_ref, precond_ref, resid_ref, update_ref,
        potential_ref, coupled_ref, work_ref, pick_ref, resid_out, update_out, potential_out,
    )
    scaled_rows(potential_out[...] * scale_ref[...], to_row_ref, 256, row_ref)
    both = products(row_ref, to_col_ref, 256)

    def deposited(k):
        return both[(k % 4) * TORSO : (k % 4 + 1) * TORSO, (k // 4) * LANES : (k // 4 + 1) * LANES]

    own_out[...] = deposited(0)
    across_out[...] = deposited(1)
    far_out[...] = deposited(2)
    for k in range(3):
        partner_out[k * TORSO : (k + 1) * TORSO, :] = deposited(3 + k)
    for k in range(2):
        next_out[k * TORSO : (k + 1) * TORSO, :] = deposited(6 + k)


def source_kernel(
    here_ref, weight_ref, own_ref, across_ref, far_ref, partner_ref, next_ref, handed_ref,
    source_out, block_out,
):
    source = own_ref[...] + across_ref[...] + far_ref[...] + partner_ref[0:TORSO]
    source = source + next_ref[TORSO:] + handed_ref[...]
    source_out[...] = source
    share = jnp.sum(jnp.sum(source * weight_ref[...], axis=0, keepdims=True), axis=1, keepdims=True)
    block_out[:, 0:LANES] = jnp.broadcast_to(share, (block_out.shape[0], LANES))
    peer = lax.broadcasted_iota(jnp.int32, (block_out.shape[0], LANES), 0)
    me = here_ref[0]
    for k in range(2):
        behind = jnp.where(peer == me - 1, source[k : k + 1], 0.0)
        ahead = jnp.where(peer == me + 1, source[TORSO - 2 + k : TORSO - 1 + k], behind)
        block_out[:, (1 + k) * LANES : (2 + k) * LANES] = ahead


def field_kernel(here_ref, block_ref, source_ref, conduct_ref, smallest_ref, out_ref, wide_ref):
    me = here_ref[0]
    devices = block_ref.shape[0]
    total = jnp.sum(jnp.sum(block_ref[:, 0:1], axis=0, keepdims=True), axis=1, keepdims=True)
    peer = lax.broadcasted_iota(jnp.int32, (devices, LANES), 0)
    wide_ref[...] = jnp.zeros_like(wide_ref)
    wide_ref[8 : 8 + TORSO, :] = source_ref[...]
    for k in range(2):
        rows = block_ref[:, (1 + k) * LANES : (2 + k) * LANES]
        above = jnp.sum(jnp.where(peer == me - 1, rows, 0.0), axis=0, keepdims=True)
        below = jnp.sum(jnp.where(peer == me + 1, rows, 0.0), axis=0, keepdims=True)
        wide_ref[6 + k : 7 + k, :] = above
        wide_ref[8 + TORSO + k : 9 + TORSO + k, :] = below
    field = torso_solve(
        wide_ref[...], conduct_ref[...], smallest_ref[0:1, 0:1], me == 0, me == devices - 1
    )
    out_ref[...] = field[8 : 8 + TORSO] - total * (1.0 / (devices * TORSO * LANES))


def call(kernel, outs, scratch, smem, flops, args, space=pltpu.VMEM):
    spec = [pl.BlockSpec(memory_space=pltpu.SMEM)] * smem
    if space == pltpu.HBM:
        args = [pltpu.with_memory_space_constraint(x, space) for x in args]
    spec += [pl.BlockSpec(memory_space=space)] * (len(args) - smem)
    return pl.pallas_call(
        kernel,
        out_shape=[s if isinstance(s, jax.ShapeDtypeStruct) else jax.ShapeDtypeStruct(s, F32) for s in outs],
        in_specs=spec,
        out_specs=[pl.BlockSpec(memory_space=pltpu.VMEM)] * len(outs),
        scratch_shapes=scratch,
        compiler_params=pltpu.CompilerParams(vmem_limit_bytes=24 * 1024 * 1024),
        cost_estimate=pl.CostEstimate(flops=flops, bytes_accessed=1 << 20, transcendentals=0),
    )(*args)


def place(i):
    return [i // 32, (i // 8) % 4, (i // 2) % 4, i % 2]


def index(c):
    return ((c[0] * 4 + c[1]) * 4 + c[2]) * 2 + c[3]


def permuted(x, move):
    return lax.ppermute(x, AXES, [(i, index(move(place(i)))) for i in range(128)])


def other_core(c):
    return c[:3] + [1 - c[3]]


def swapped(axis, pairing):
    partner = ((1, 0, 3, 2), (3, 2, 1, 0), (2, 3, 0, 1))[pairing]

    def move(c):
        c = list(c)
        c[axis] = partner[c[axis]]
        return c

    return move


def combined(parts, rows):
    total = parts[0]
    for part in parts[1:]:
        total = total + part
    if rows == total.shape[0]:
        return total
    least = parts[0]
    for part in parts[1:]:
        least = jnp.minimum(least, part)
    line = lax.broadcasted_iota(jnp.int32, total.shape, 0)
    return jnp.where(line < rows, total, least)


RING_ORDER = (2, 1, 0)


def over_all(x):
    for axis in range(3):
        parts = [x]
        for k in RING_ORDER:
            parts.append(permuted(x, swapped(axis, k)))
        x = combined(parts, SLOT_ROWS)
        if axis == 1:
            x = combined([x, permuted(x, other_core)], SLOT_ROWS)
    return x


def near(i, devices):
    return (i + 1 if i % 2 else i - 1) % devices


def from_behind(x, by, count):
    return lax.ppermute(x, AXES, [(i, (i + by) % count) for i in range(count)])


def body(
    states, region, half_volt, slopes, rates, conductance, reversal, stiffness, preconditioner,
    slots, slot_gain, owner, cell, source_gain, torso_conduct,
):
    devices = lax.axis_size(AXES)
    here = lax.axis_index(AXES)
    node = (TILES, LANES)
    tile = (TORSO, LANES)
    grid = (SLOT_ROWS, LANES)
    region, slots, owner, cell, source_gain = (
        x.reshape(node) for x in (region, slots, owner, cell, source_gain)
    )
    gain = slot_gain.reshape(grid)
    whom = jnp.stack([here, jnp.int32(devices)]).astype(jnp.int32)
    rowspace = pltpu.VMEM((256, 4096), BF16)
    colspace = pltpu.VMEM((128, 4096), BF16)
    nodespace = pltpu.VMEM(node, F32)
    tablespace = pltpu.VMEM((3, 18), F32)
    indexspace = pltpu.VMEM(node, jnp.int32)

    pick = jax.ShapeDtypeStruct((128, 4096), BF16)
    target = jax.ShapeDtypeStruct((256, 4096), BF16)
    new_states, resid, update, payload, slots, gain, preconditioner, picks, top, bottom = call(
        ionic_kernel,
        [states.shape, node, node, (PAYLOAD, LANES), jax.ShapeDtypeStruct(node, jnp.int32), grid,
         preconditioner.shape, pick, (8, LANES), (8, LANES)],
        [pltpu.VMEM(states.shape, F32), indexspace] + [tablespace] * 5
        + [pltpu.VMEM(tile, F32), pltpu.VMEM((128, 128), F32), nodespace, rowspace,
           colspace, pltpu.SemaphoreType.DMA((11,))],
        0, 40000000,
        (states, region, half_volt, slopes, rates, conductance, reversal, slots, torso_conduct,
         gain, preconditioner),
        pltpu.HBM,
    )
    even = here % 2 == 0
    inner = permuted(jnp.where(even, bottom, top), other_core)
    outer = jnp.where(even, top, bottom)
    outer = lax.ppermute(
        outer, AXES,
        [(i, i if i in (0, devices - 1) else near(i, devices)) for i in range(devices)],
    )
    conduct = jnp.concatenate(
        [jnp.where(even, outer, inner), torso_conduct, jnp.where(even, inner, outer)], axis=0
    )
    payload = over_all(payload)
    resid, update, potential, payload, smallest = call(
        first_step_kernel,
        [node, node, node, grid, (8, LANES)],
        [nodespace, nodespace, rowspace, colspace],
        0, 40000000,
        (payload, gain, slots, preconditioner, picks, resid, update),
    )
    (weight,) = call(weight_kernel, [tile], [], 1, 4000000, (whom, smallest, conduct))
    to_row, to_col = call(
        target_kernel, [target, target], [], 1, 10000000, (whom, smallest, owner, cell)
    )
    payload = over_all(payload)
    resid, update, potential, payload = call(
        second_step_kernel,
        [node, node, node, grid],
        [nodespace, nodespace, rowspace, colspace],
        0, 40000000,
        (payload, gain, slots, preconditioner, picks, resid, update, potential),
    )
    payload = over_all(payload)
    potential, own, across, far, partner, nearby = call(
        last_step_kernel,
        [node, tile, tile, tile, (3 * TORSO, LANES), (2 * TORSO, LANES)],
        [nodespace, nodespace, nodespace, nodespace, pltpu.VMEM((512, 4096), BF16)],
        0, 40000000,
        (payload, gain, slots, preconditioner, picks, resid, update, potential,
         to_row, to_col, source_gain),
    )
    far = lax.ppermute(far, AXES, [(i, (i + 3 if i % 2 else i - 3) % devices) for i in range(devices)])
    across = from_behind(across, devices // 2, devices)
    partner = permuted(partner, other_core)
    nearby = lax.ppermute(
        nearby + partner[TORSO:], AXES, [(i, near(i, devices)) for i in range(devices)]
    )
    handed = permuted(nearby[:TORSO], other_core)
    source, blocks = call(
        source_kernel,
        [tile, (devices, 3 * LANES)],
        [], 1, 1000000,
        (whom, weight, own, across, far, partner, nearby, handed),
    )
    blocks = lax.all_to_all(blocks, AXES, 0, 0, tiled=True)
    (grounded,) = call(
        field_kernel, [tile], [pltpu.VMEM((TORSO + 16, LANES), F32)], 1, 4000000,
        (whom, blocks, source, conduct, smallest),
    )
    return new_states, potential.reshape(-1), grounded


def solution(mesh):
    torus = Mesh(mesh.devices.reshape(4, 4, 4, 2), AXES)
    dom = P(AXES)
    placed = (
        P(None, AXES), dom, P(), P(), P(), P(), P(), P(AXES, None, None), P(AXES, None, None),
        dom, P(), P(AXES, None), dom, dom, P(AXES, None),
    )
    return jax.shard_map(
        body, mesh=torus, in_specs=placed, out_specs=(P(None, AXES), dom, P(AXES, None)), check_vma=False
    )
```
